128 devices in a mesh: frame: 32 (over y, z, x_lo), group: 4 (over x_hi, core).
Axes of the slice: x: 4 (x_hi: 2, x_lo: 2; x = x_hi * 2 + x_lo), y: 4, z: 4, core: 2. Of those that a mesh axis runs over, the one named last changes fastest.
Arguments:
- frames: bfloat16 [128, 64, 1920], P(('frame', 'group')), may hold values from -16 to 16
- motion: int32 [128, 2, 4, 120], P(('frame', 'group')), may hold values from -64 to 64
- weights: int32 [128, 4, 120], P(('frame', 'group')), may hold values from 1 to 16
- strip_map: int32 [128], replicated, may hold values from 0 to 127, each once
- prior_image: float32 [128, 1, 3840], P(('frame', 'group')), may hold values from -6 to 6
- prior_weight: float32 [128, 1, 3840], P(('frame', 'group')), may hold values from 100 to 2000
Outputs:
- joined_image: float32 [128, 1, 3840], P(('frame', 'group'))
The draws below stay inside these ranges and needn't reach their ends.
Inputs may be any that keep to these rules, and one draw needn't show every extreme that they name: `motion`: motion offsets are whole numbers in high-resolution pixels. `strip_map`: each strip number appears exactly once.
All inputs are finite; a program needn't handle non-finite values.
Results may differ from the reference program's by a relative error of at most 0.0003.
Values sent between devices are 32-bit elements; how exact they have to be, the bound alone decides.
No kernel may reach another device: no remote copies, remote signals or barrier semaphores. Data moves between devices by JAX's collectives and lax.ppermute only.
A program may use at most 256 MiB of HBM per device.

```python
import math
import jax
import jax.numpy as jnp
from jax import lax

FRAME_ROWS = 64
FRAME_COLS = 1920
MAX_SHIFT = 64
FRAMES = 128
STRIPS = 128
GRID_COLS = 3840
STRIP_ROWS = 1


def set_ends(values, key, low, largest):
    shape = values.shape
    place = [jax.random.randint(jax.random.fold_in(key, axis), (), 0, shape[axis]) for axis in range(len(shape))]
    values = values.at[tuple(place)].set(low)
    longest = shape.index(max(shape))
    place[longest] = (place[longest] + 1) % shape[longest]
    return values.at[tuple(place)].set(largest)


def raised(values, rng, source, target, shards_of, factor):
    owner, partner = [(jnp.arange(values.shape[position]) // (values.shape[position] // shards_of)).reshape([-1 if axis == position else 1 for axis in range(values.ndim)]) for position in (source, target)]
    chosen = jax.random.permutation(rng, shards_of)[partner]
    strong = (owner == chosen) | (owner == (partner + shards_of // 2) % shards_of)
    return jnp.where(strong, factor * values, values)


def level_of(rng, shape, cuts, least, largest):
    level = 1.0
    for axis_at, blocks in cuts:
        heights = jax.random.uniform(jax.random.fold_in(jax.random.fold_in(rng, 6), axis_at), (blocks,), jnp.float32, least / len(cuts), largest / len(cuts))
        level = level * jnp.repeat(jnp.exp(heights), shape[axis_at] // blocks).reshape((-1,) + (1,) * (len(shape) - 1 - axis_at))
    return level


def normal_values(key, extent, deviation, limit, split=(), kind=jnp.bfloat16):
    array = jax.random.normal(key, extent, jnp.float32) * deviation
    if len(split) > 0:
        array = level_of(key, extent, split, -0.22, 0.18) * array
    return jnp.clip(array, min=-limit, max=limit).astype(kind)


def heavy_noise(stream_key, extent, spread, limit, pieces, heavy, kind=jnp.bfloat16):
    result = spread * jax.random.normal(stream_key, extent, jnp.float32)
    if pieces:
        result = result * level_of(stream_key, extent, pieces, -0.22, 0.18)
    return jnp.clip(raised(result, jax.random.fold_in(stream_key, 3), *heavy), -limit, limit).astype(kind)


def setup_inputs(seed: int = 0) -> dict:
    key_of = jax.random.split(jax.random.key(seed), 7)
    frames = heavy_noise(key_of[0], (FRAMES, FRAME_ROWS, FRAME_COLS), 1.0, 16.0, ((0, 128),), (0, 1, 64, 4.0))
    motion = set_ends(jax.random.randint(key_of[1], (FRAMES, 2, FRAME_ROWS // 16, FRAME_COLS // 16), 0 - MAX_SHIFT, MAX_SHIFT + 1), jax.random.fold_in(key_of[1], 1), 0 - MAX_SHIFT, MAX_SHIFT).astype(jnp.int32)
    weights = set_ends(jax.random.randint(key_of[2], (FRAMES, FRAME_ROWS // 16, FRAME_COLS // 16), 1, 17), jax.random.fold_in(key_of[2], 1), 1, 16).astype(jnp.int32)
    strip_map = jax.random.permutation(key_of[3], STRIPS).astype(jnp.int32)
    prior_image = normal_values(key_of[4], (STRIPS, STRIP_ROWS, GRID_COLS), 1.0, 6.0, ((0, 128),), jnp.float32)
    prior_weight = jnp.clip(jnp.exp(math.log(2000.0) - 2.9957323 * jax.random.uniform(key_of[5], (STRIPS, STRIP_ROWS, GRID_COLS), jnp.float32) ** level_of(key_of[5], (STRIPS, STRIP_ROWS, GRID_COLS), ((0, 128),), -0.2, 0.2)), 100.0, 2000.0)
    return {"frames": frames, "motion": motion, "weights": weights, "strip_map": strip_map, "prior_image": prior_image, "prior_weight": prior_weight}


def upsample(low_frame):
    signal = low_frame.astype(jnp.float32)
    upper_row = jnp.concatenate([signal[:1], signal[:-1]], axis=0)
    lower_row = jnp.concatenate([signal[1:], signal[-1:]], axis=0)
    signal = jnp.stack([0.75 * signal + 0.25 * upper_row, 0.75 * signal + 0.25 * lower_row], axis=1)
    signal = signal.reshape(2 * low_frame.shape[0], low_frame.shape[1])
    left_col = jnp.concatenate([signal[:, :1], signal[:, :-1]], axis=1)
    right_col = jnp.concatenate([signal[:, 1:], signal[:, -1:]], axis=1)
    signal = jnp.stack([0.75 * signal + 0.25 * left_col, 0.75 * signal + 0.25 * right_col], axis=2)
    return signal.reshape(signal.shape[0], 2 * low_frame.shape[1])


def targets(shifts, weight, frame_rows, frame_cols):
    grid_rows = 2 * frame_rows
    grid_cols = 2 * frame_cols
    shift_rows = jnp.repeat(jnp.repeat(shifts[0], 32, axis=0), 32, axis=1).astype(jnp.int32)
    shift_cols = jnp.repeat(jnp.repeat(shifts[1], 32, axis=0), 32, axis=1).astype(jnp.int32)
    weight_map = jnp.repeat(jnp.repeat(weight, 32, axis=0), 32, axis=1).astype(jnp.float32)
    target_rows = jnp.arange(grid_rows, dtype=jnp.int32)[:, None] + shift_rows
    target_cols = jnp.arange(grid_cols, dtype=jnp.int32)[None, :] + shift_cols
    in_grid = (target_rows >= 0) & (target_rows < grid_rows) & (target_cols >= 0) & (target_cols < grid_cols)
    flat_index = jnp.where(in_grid, target_rows * grid_cols + target_cols, grid_rows * grid_cols)
    return flat_index.reshape(-1).astype(jnp.int32), weight_map.reshape(-1)


def reference(frames, motion, weights, strip_map, prior_image, prior_weight):
    frame_rows = frames.shape[1]
    frame_cols = frames.shape[2]
    grid_cells = 4 * frame_rows * frame_cols

    def add_frame(running, frame_item):
        low_frame, shifts, weight = frame_item
        flat_index, weight_map = targets(shifts, weight, frame_rows, frame_cols)
        values = upsample(low_frame).reshape(-1) * weight_map
        weighted = running[0].at[flat_index].add(values, mode="drop")
        counts = running[1].at[flat_index].add(weight_map, mode="drop")
        return (weighted, counts), None

    initial = (jnp.zeros((grid_cells,), jnp.float32), jnp.zeros((grid_cells,), jnp.float32))
    (weighted, counts), _ = lax.scan(add_frame, initial, (frames, motion, weights))
    strips = strip_map.shape[0]
    strip_order = strip_map.astype(jnp.int32)
    weighted = jnp.take(weighted.reshape(strips, -1, 2 * frame_cols), strip_order, axis=0)
    counts = jnp.take(counts.reshape(strips, -1, 2 * frame_cols), strip_order, axis=0)
    return (weighted + prior_weight * prior_image) / (counts + prior_weight)
```

```python
import jax
import jax.numpy as jnp
from jax import lax
from jax.experimental import pallas as pl
from jax.experimental.pallas import tpu as pltpu
from jax.sharding import PartitionSpec as P

MAX_SHIFT = 64
AXES = ("frame", "group")
LANES = 128
BLOCK = 32
HALF = 64
PITCH = 36


def splat_kernel(motion, weights, order, frame, out, low, acc, edge, joined):
    low_rows, low_cols = frame.shape
    bands = low_rows // 16
    tiles = 2 * low_cols // LANES
    windows = acc.shape[0] // 2
    grid_rows = 2 * low_rows
    margin = MAX_SHIFT // 2
    lane = lax.broadcasted_iota(jnp.int32, (8, LANES), 1)

    def clear(i, carry):
        acc[i] = jnp.zeros(acc.shape[1:], jnp.float32)
        return carry

    lax.fori_loop(0, acc.shape[0], clear, 0)

    def clear_edge(i, carry):
        edge[pl.ds(pl.multiple_of(i * 64, 64), 64), :] = jnp.zeros((64, LANES), jnp.float32)
        return carry

    lax.fori_loop(0, edge.shape[0] // 64, clear_edge, 0)

    parts = low_cols // LANES
    cols = [frame[:, LANES * m : LANES * (m + 1)] for m in range(parts)]
    first = jnp.broadcast_to(frame[:, :1], (low_rows, LANES))
    last = jnp.broadcast_to(frame[:, low_cols - 1 :], (low_rows, LANES))
    source = jnp.concatenate(
        [jnp.concatenate([first] + cols[:-1], 0), jnp.concatenate(cols, 0), jnp.concatenate(cols[1:] + [last], 0)], 1
    )
    tap = lax.broadcasted_iota(jnp.int32, (3 * LANES, 2 * LANES), 0) - LANES
    target = lax.broadcasted_iota(jnp.int32, (3 * LANES, 2 * LANES), 1)
    near = target >> 1
    far = near + 2 * (target & 1) - 1
    stretch = jnp.where(tap == near, 0.75, jnp.where(tap == far, 0.25, 0.0)).astype(jnp.bfloat16)
    wide = jnp.dot(source, stretch, preferred_element_type=jnp.float32)
    for m in range(parts):
        for h in range(2):
            piece = wide[low_rows * m : low_rows * (m + 1), LANES * h : LANES * (h + 1)]
            low[2 * m + h, 8 : 8 + low_rows, :] = piece
            low[2 * m + h, 7:8, :] = piece[:1]
            low[2 * m + h, 8 + low_rows : 9 + low_rows, :] = piece[low_rows - 1 :]

    def column(n, carry):
        for b in range(bands):
            base = 8 + 16 * b
            mid = 0.75 * low[n, base : base + 16, :]
            even = mid + 0.25 * low[n, base - 1 : base + 15, :]
            odd = mid + 0.25 * low[n, base + 1 : base + 17, :]
            for q in range(LANES // BLOCK):
                j = n * (LANES // BLOCK) + q
                dy = motion[0, b, j]
                dx = motion[1, b, j]
                w = weights[b, j].astype(jnp.float32)
                start = dx + n * LANES + (BLOCK * q + HALF)
                u = start >> 6
                shift = ((start & 63) - BLOCK * q) & 127
                gain = pltpu.roll(jnp.where(lane // BLOCK == q, w, 0.0), shift, 1)
                gains = jnp.concatenate([gain, gain], 0)
                par = dy & 1
                he = margin + 16 * b + (dy >> 1)
                ho = margin + 16 * b + ((dy + 1) >> 1)
                acc[par * windows + u, pl.ds(he, 16), :] += pltpu.roll(even, shift, 1) * gains
                acc[(1 - par) * windows + u, pl.ds(ho, 16), :] += pltpu.roll(odd, shift, 1) * gains
                cell = (u & 1) * 32 + (u >> 1)
                r0 = jnp.clip(32 * b + dy, 0, grid_rows) * 64 + cell
                r1 = jnp.clip(32 * b + dy + 32, 0, grid_rows) * 64 + cell
                edge[pl.ds(r0, 1), :] += gain[:1]
                edge[pl.ds(r1, 1), :] -= gain[:1]
        return carry

    lax.fori_loop(0, tiles, column, 0)

    left = lax.broadcasted_iota(jnp.int32, (low_rows, LANES), 1) < HALF

    def join(k, carry):
        for p in range(2):
            here = acc[p * windows + 2 * k + 1, margin : margin + low_rows, :]
            before = acc[p * windows + 2 * k, margin : margin + low_rows, :]
            after = acc[p * windows + 2 * k + 2, margin : margin + low_rows, :]
            whole = here + pltpu.roll(jnp.where(left, after, before), HALF, 1)
            joined[pl.ds(p * low_rows * PITCH + k, low_rows, stride=PITCH), :] = whole
        return carry

    lax.fori_loop(0, tiles, join, 0)

    left32 = lax.broadcasted_iota(jnp.int32, (32, LANES), 1) < HALF
    zero = jnp.zeros((32, LANES), jnp.float32)

    def counts(r, carry):
        here, before, after = carry
        here = here + edge[pl.ds(pl.multiple_of(r * 64, 64) + 32, 32), :]
        before = before + edge[pl.ds(pl.multiple_of(r * 64, 64), 32), :]
        after = after + edge[pl.ds(pl.multiple_of(r * 64, 64) + 1, 32), :]
        joined[pl.ds(2 * low_rows * PITCH + r * 32, 32), :] = here + pltpu.roll(
            jnp.where(left32, after, before), HALF, 1
        )
        return here, before, after

    lax.fori_loop(0, grid_rows, counts, (zero, zero, zero))

    def place(s, carry):
        row = order[s]
        out[s, :tiles, :] = joined[pl.ds(((row & 1) * low_rows + (row >> 1)) * PITCH, tiles), :]
        out[s, tiles : 2 * tiles, :] = joined[pl.ds(2 * low_rows * PITCH + row * 32, tiles), :]
        return carry

    lax.fori_loop(0, grid_rows, place, 0)


def splat(frame, motion, weights, order):
    low_rows, low_cols = frame.shape
    grid_rows = 2 * low_rows
    tiles = 2 * low_cols // LANES
    windows = 2 * tiles + 2
    return pl.pallas_call(
        splat_kernel,
        out_shape=jax.ShapeDtypeStruct((grid_rows, 2 * tiles, LANES), jnp.float32),
        in_specs=[pl.BlockSpec(memory_space=pltpu.SMEM)] * 3 + [pl.BlockSpec(memory_space=pltpu.VMEM)],
        out_specs=pl.BlockSpec(memory_space=pltpu.VMEM),
        scratch_shapes=[
            pltpu.VMEM((tiles, low_rows + 16, LANES), jnp.float32),
            pltpu.VMEM((2 * windows, grid_rows, LANES), jnp.float32),
            pltpu.VMEM(((grid_rows + 2) * 64, LANES), jnp.float32),
            pltpu.VMEM((grid_rows * (PITCH + 32), LANES), jnp.float32),
        ],
        compiler_params=pltpu.CompilerParams(vmem_limit_bytes=40 * 1024 * 1024),
        name="splat",
    )(motion, weights, order, frame)


def body(frames, motion, weights, strip_map, prior_image, prior_weight):
    tiles = 2 * frames.shape[2] // LANES
    cells = splat(frames[0], motion[0], weights[0], strip_map)
    received = lax.all_to_all(cells, AXES, 0, 0, tiled=True)
    total = received.sum(axis=0)
    sums = total[:tiles].reshape(prior_image.shape)
    counts = total[tiles:].reshape(prior_image.shape)
    return (sums + prior_weight * prior_image) / (counts + prior_weight)


def solution(mesh):
    in_specs = (
        P(AXES, None, None),
        P(AXES, None, None, None),
        P(AXES, None, None),
        P(),
        P(AXES, None, None),
        P(AXES, None, None),
    )
    return jax.shard_map(body, mesh=mesh, in_specs=in_specs, out_specs=P(AXES, None, None), check_vma=False)
```

```python
import functools

import jax
import jax.numpy as jnp
from jax import lax
from jax.experimental import pallas as pl
from jax.experimental.pallas import tpu as pltpu
from jax.sharding import PartitionSpec as P


MAX_SHIFT = 64
AXES = ("frame", "group")
LANES = 128
BLOCK = 32
HALF = 64
PITCH = 36


def device_of(x, y, z, core):
    return ((y * 4 + z) * 2 + (x & 1)) * 4 + (x >> 1) * 2 + core


def splat_kernel(motion, weights, order, frame, keep, send, low, acc, edge, joined):
    low_rows, low_cols = frame.shape
    bands = low_rows // 16
    tiles = 2 * low_cols // LANES
    windows = acc.shape[0] // 2
    grid_rows = 2 * low_rows
    margin = MAX_SHIFT // 2
    lane = lax.broadcasted_iota(jnp.int32, (8, LANES), 1)

    def clear(i, carry):
        acc[i] = jnp.zeros(acc.shape[1:], jnp.float32)
        return carry

    lax.fori_loop(0, acc.shape[0], clear, 0)

    def clear_edge(i, carry):
        edge[pl.ds(pl.multiple_of(i * 64, 64), 64), :] = jnp.zeros((64, LANES), jnp.float32)
        return carry

    lax.fori_loop(0, edge.shape[0] // 64, clear_edge, 0)

    parts = low_cols // LANES
    cols = [frame[:, LANES * m : LANES * (m + 1)] for m in range(parts)]
    first = jnp.broadcast_to(frame[:, :1], (low_rows, LANES))
    last = jnp.broadcast_to(frame[:, low_cols - 1 :], (low_rows, LANES))
    source = jnp.concatenate(
        [jnp.concatenate([first] + cols[:-1], 0), jnp.concatenate(cols, 0), jnp.concatenate(cols[1:] + [last], 0)], 1
    )
    tap = lax.broadcasted_iota(jnp.int32, (3 * LANES, 2 * LANES), 0) - LANES
    target = lax.broadcasted_iota(jnp.int32, (3 * LANES, 2 * LANES), 1)
    near = target >> 1
    far = near + 2 * (target & 1) - 1
    stretch = jnp.where(tap == near, 0.75, jnp.where(tap == far, 0.25, 0.0)).astype(jnp.bfloat16)
    wide = jnp.dot(source, stretch, preferred_element_type=jnp.float32)
    for m in range(parts):
        for h in range(2):
            piece = wide[low_rows * m : low_rows * (m + 1), LANES * h : LANES * (h + 1)]
            low[2 * m + h, 8 : 8 + low_rows, :] = piece
            low[2 * m + h, 7:8, :] = piece[:1]
            low[2 * m + h, 8 + low_rows : 9 + low_rows, :] = piece[low_rows - 1 :]

    def column(n, carry):
        for b in range(bands):
            base = 8 + 16 * b
            mid = 0.75 * low[n, base : base + 16, :]
            even = mid + 0.25 * low[n, base - 1 : base + 15, :]
            odd = mid + 0.25 * low[n, base + 1 : base + 17, :]
            for q in range(LANES // BLOCK):
                j = n * (LANES // BLOCK) + q
                dy = motion[0, b, j]
                dx = motion[1, b, j]
                w = weights[b, j].astype(jnp.float32)
                start = dx + n * LANES + (BLOCK * q + HALF)
                u = start >> 6
                shift = ((start & 63) - BLOCK * q) & 127
                gain = pltpu.roll(jnp.where(lane // BLOCK == q, w, 0.0), shift, 1)
                gains = jnp.concatenate([gain, gain], 0)
                par = dy & 1
                he = margin + 16 * b + (dy >> 1)
                ho = margin + 16 * b + ((dy + 1) >> 1)
                acc[par * windows + u, pl.ds(he, 16), :] += pltpu.roll(even, shift, 1) * gains
                acc[(1 - par) * windows + u, pl.ds(ho, 16), :] += pltpu.roll(odd, shift, 1) * gains
                cell = (u & 1) * 32 + (u >> 1)
                r0 = jnp.clip(32 * b + dy, 0, grid_rows) * 64 + cell
                r1 = jnp.clip(32 * b + dy + 32, 0, grid_rows) * 64 + cell
                edge[pl.ds(r0, 1), :] += gain[:1]
                edge[pl.ds(r1, 1), :] -= gain[:1]
        return carry

    lax.fori_loop(0, tiles, column, 0)

    left = lax.broadcasted_iota(jnp.int32, (low_rows, LANES), 1) < HALF

    def join(step, carry):
        for i in range(3):
            k = step * 3 + i
            for p in range(2):
                here = acc[p * windows + 2 * k + 1, margin : margin + low_rows, :]
                before = acc[p * windows + 2 * k, margin : margin + low_rows, :]
                after = acc[p * windows + 2 * k + 2, margin : margin + low_rows, :]
                whole = here + pltpu.roll(jnp.where(left, after, before), HALF, 1)
                joined[pl.ds(p * low_rows * PITCH + k, low_rows, stride=PITCH), :] = whole
        return carry

    lax.fori_loop(0, tiles // 3, join, 0)

    left32 = lax.broadcasted_iota(jnp.int32, (32, LANES), 1) < HALF
    zero = jnp.zeros((32, LANES), jnp.float32)

    def counts(step, carry):
        here, before, after = carry
        for i in range(8):
            at = pl.multiple_of((step * 8 + i) * 64, 64)
            here = here + edge[pl.ds(at + 32, 32), :]
            before = before + edge[pl.ds(at, 32), :]
            after = after + edge[pl.ds(at + 1, 32), :]
            slot = pl.multiple_of(2 * low_rows * PITCH + (step * 8 + i) * 32, 32)
            joined[pl.ds(slot, 32), :] = here + pltpu.roll(jnp.where(left32, after, before), HALF, 1)
        return here, before, after

    lax.fori_loop(0, grid_rows // 8, counts, (zero, zero, zero))

    spot = lax.axis_index("frame")
    side = lax.axis_index("group")
    my_x, my_y, my_z, my_core = (side >> 1) * 2 + (spot & 1), spot >> 3, (spot >> 1) & 3, side & 1
    half_rows = keep.shape[0] // 2

    def place(t, carry):
        dx, dy, dz = t >> 4, (t >> 2) & 3, t & 3
        chip = device_of((my_x + dx) & 3, (my_y + dy) & 3, (my_z + dz) & 3, 0)
        first_slot = t * tiles
        second_slot = half_rows + (dy * 16 + dx * 4 + dz) * tiles
        for ref, core in ((keep, my_core), (send, 1 - my_core)):
            row = order[chip + core]
            ref[pl.ds(first_slot, tiles), :] = joined[
                pl.ds(((row & 1) * low_rows + (row >> 1)) * PITCH, tiles), :
            ]
            ref[pl.ds(second_slot, tiles), :] = joined[pl.ds(2 * low_rows * PITCH + row * 32, tiles), :]
        return carry

    lax.fori_loop(0, grid_rows // 2, place, 0)


def splat(frame, motion, weights, order):
    low_rows, low_cols = frame.shape
    grid_rows = 2 * low_rows
    tiles = 2 * low_cols // LANES
    windows = 2 * tiles + 2
    return pl.pallas_call(
        splat_kernel,
        out_shape=[jax.ShapeDtypeStruct((grid_rows * tiles, LANES), jnp.float32)] * 2,
        in_specs=[pl.BlockSpec(memory_space=pltpu.SMEM)] * 3 + [pl.BlockSpec(memory_space=pltpu.VMEM)],
        out_specs=[pl.BlockSpec(memory_space=pltpu.VMEM)] * 2,
        scratch_shapes=[
            pltpu.VMEM((tiles, low_rows + 16, LANES), jnp.float32),
            pltpu.VMEM((2 * windows, grid_rows, LANES), jnp.float32),
            pltpu.VMEM(((grid_rows + 2) * 64, LANES), jnp.float32),
            pltpu.VMEM((grid_rows * (PITCH + 32), LANES), jnp.float32),
        ],
        compiler_params=pltpu.CompilerParams(vmem_limit_bytes=40 * 1024 * 1024),
        name="splat",
    )(motion, weights, order, frame)


def split_kernel(parts, *refs):
    ins, outs = refs[: len(refs) - parts], refs[len(refs) - parts :]
    rows = outs[0].shape[0]
    for i, out in enumerate(outs):
        total = ins[0][i * rows : (i + 1) * rows, :]
        for ref in ins[1:]:
            total = total + ref[i * rows : (i + 1) * rows, :]
        out[...] = total


def fold(name, terms, parts):
    rows = terms[0].shape[0] // parts
    return pl.pallas_call(
        functools.partial(split_kernel, parts),
        out_shape=[jax.ShapeDtypeStruct((rows, LANES), jnp.float32)] * parts,
        in_specs=[pl.BlockSpec(memory_space=pltpu.VMEM)] * len(terms),
        out_specs=[pl.BlockSpec(memory_space=pltpu.VMEM)] * parts,
        compiler_params=pltpu.CompilerParams(vmem_limit_bytes=12 * 1024 * 1024),
        name=name,
    )(*terms)


def moved(value, dx, dy, dz, flip=0):
    pairs = []
    for x in range(4):
        for y in range(4):
            for z in range(4):
                for core in range(2):
                    pairs.append(
                        (device_of(x, y, z, core), device_of((x + dx) % 4, (y + dy) % 4, (z + dz) % 4, core ^ flip))
                    )
    return lax.ppermute(value, AXES, pairs)


def body(frames, motion, weights, strip_map, prior_image, prior_weight):
    tiles = 2 * frames.shape[2] // LANES
    keep, send = splat(frames[0], motion[0], weights[0], strip_map)
    other = moved(send, 0, 0, 0, flip=1)
    parts = fold("fold_core", [keep, other], 8)
    weighted, counted = list(parts[:4]), list(parts[4:])
    for d in range(1, 4):
        weighted[d] = moved(weighted[d], d, 0, 0)
        counted[d] = moved(counted[d], 0, d, 0)
    weighted = list(fold("fold_first", weighted, 4))
    counted = list(fold("fold_second", counted, 4))
    for d in range(1, 4):
        weighted[d] = moved(weighted[d], 0, d, 0)
        counted[d] = moved(counted[d], d, 0, 0)
    weighted = sum(weighted[1:], weighted[0]).reshape(4, tiles, LANES)
    counted = sum(counted[1:], counted[0]).reshape(4, tiles, LANES)
    both = jnp.concatenate([weighted, counted], axis=1)
    total = both[0]
    for d in range(1, 4):
        total = total + moved(both[d], 0, 0, d)
    sums = total[:tiles].reshape(prior_image.shape)
    counts = total[tiles:].reshape(prior_image.shape)
    return (sums + prior_weight * prior_image) / (counts + prior_weight)


def solution(mesh):
    in_specs = (
        P(AXES, None, None),
        P(AXES, None, None, None),
        P(AXES, None, None),
        P(),
        P(AXES, None, None),
        P(AXES, None, None),
    )
    return jax.shard_map(body, mesh=mesh, in_specs=in_specs, out_specs=P(AXES, None, None), check_vma=False)
```

```python
import functools

import jax
import jax.numpy as jnp
from jax import lax
from jax.experimental import pallas as pl
from jax.experimental.pallas import tpu as pltpu
from jax.sharding import PartitionSpec as P


MAX_SHIFT = 64
AXES = ("frame", "group")
LANES = 128
BLOCK = 32
HALF = 64
PITCH = 36


def device_of(x, y, z, core):
    return ((y * 4 + z) * 2 + (x & 1)) * 4 + (x >> 1) * 2 + core


def splat_kernel(
    motion_in, weights_in, order_in, frame_in, keep, send,
    motion, weights, order, frame, fields, table, low, acc, edge, joined, sems,
):
    low_rows, low_cols = frame.shape
    bands, blocks = weights.shape
    tiles = 2 * low_cols // LANES
    windows = 2 * tiles + 2
    grid_rows = 2 * low_rows
    span = grid_rows
    margin = MAX_SHIFT // 2
    copies = [
        pltpu.make_async_copy(source, target, sems.at[i])
        for i, (source, target) in enumerate(
            ((motion_in, motion), (weights_in, weights), (order_in, order), (frame_in, frame))
        )
    ]
    for copy in copies:
        copy.start()

    def clear(i, carry):
        for k in range(4):
            at = pl.multiple_of((i * 4 + k) * span, span) + margin
            acc[pl.ds(at, low_rows), :] = jnp.zeros((low_rows, LANES), jnp.float32)
        return carry

    lax.fori_loop(0, windows // 2, clear, 0)

    for copy in copies[:3]:
        copy.wait()
    band = lax.broadcasted_iota(jnp.int32, (bands, blocks), 0)
    block = lax.broadcasted_iota(jnp.int32, (bands, blocks), 1)
    dy, dx = motion[0], motion[1]
    window = (dx + BLOCK * block + HALF) >> 6
    par = dy & 1
    top = margin + 16 * band
    cell = (window & 1) * 32 + (window >> 1)
    entries = (
        (par * windows + window) * span + top + (dy >> 1),
        ((1 - par) * windows + window) * span + top + ((dy + 1) >> 1),
        dx & (LANES - 1),
        jnp.clip(BLOCK * band + dy, 0, grid_rows) * 64 + cell,
        jnp.clip(BLOCK * band + dy + BLOCK, 0, grid_rows) * 64 + cell,
        weights[...],
    )
    for f, entry in enumerate(entries):
        fields[f, :, :blocks] = entry
    row = order[...]
    fields[len(entries), :1, :] = ((row & 1) * low_rows + (row >> 1)) * PITCH

    def clear_edge(i, carry):
        at = pl.multiple_of(i * 512, 512)
        edge[pl.ds(at, 512), :] = jnp.zeros((512, LANES), jnp.float32)
        return carry

    lax.fori_loop(0, grid_rows * 64 // 512, clear_edge, 0)

    to_scalar = pltpu.make_async_copy(fields, table, sems.at[4])
    to_scalar.start()
    copies[3].wait()

    parts = low_cols // LANES
    cols = [frame[:, LANES * m : LANES * (m + 1)] for m in range(parts)]
    first = jnp.broadcast_to(frame[:, :1], (low_rows, LANES))
    last = jnp.broadcast_to(frame[:, low_cols - 1 :], (low_rows, LANES))
    source = jnp.concatenate(
        [jnp.concatenate([first] + cols[:-1], 0), jnp.concatenate(cols, 0), jnp.concatenate(cols[1:] + [last], 0)], 1
    )
    tap = lax.broadcasted_iota(jnp.int32, (3 * LANES, 2 * LANES), 0) - LANES
    target = lax.broadcasted_iota(jnp.int32, (3 * LANES, 2 * LANES), 1)
    near = target >> 1
    far = near + 2 * (target & 1) - 1
    stretch = jnp.where(tap == near, 0.75, jnp.where(tap == far, 0.25, 0.0)).astype(jnp.bfloat16)
    wide = jnp.dot(source, stretch, preferred_element_type=jnp.float32)
    for m in range(parts):
        for h in range(2):
            piece = wide[low_rows * m : low_rows * (m + 1), LANES * h : LANES * (h + 1)]
            low[2 * m + h, 8 : 8 + low_rows, :] = piece
            low[2 * m + h, 7:8, :] = piece[:1]
            low[2 * m + h, 8 + low_rows : 9 + low_rows, :] = piece[low_rows - 1 :]
    to_scalar.wait()

    owner = lax.broadcasted_iota(jnp.int32, (8, LANES), 1) // BLOCK

    def column(n, carry):
        for b in range(bands):
            base = 8 + 16 * b
            mid = 0.75 * low[n, base : base + 16, :]
            even = mid + 0.25 * low[n, base - 1 : base + 15, :]
            odd = mid + 0.25 * low[n, base + 1 : base + 17, :]
            for q in range(LANES // BLOCK):
                j = n * (LANES // BLOCK) + q
                at_even, at_odd, shift, at_first, at_end, w = (table[f, b, j] for f in range(6))
                gain = pltpu.roll(jnp.where(owner == q, w.astype(jnp.float32), 0.0), shift, 1)
                gains = jnp.concatenate([gain, gain], 0)
                acc[pl.ds(at_even, 16), :] += pltpu.roll(even, shift, 1) * gains
                acc[pl.ds(at_odd, 16), :] += pltpu.roll(odd, shift, 1) * gains
                edge[pl.ds(at_first, 1), :] += gain[:1]
                edge[pl.ds(at_end, 1), :] -= gain[:1]
        return carry

    lax.fori_loop(0, tiles, column, 0)

    left = lax.broadcasted_iota(jnp.int32, (low_rows, LANES), 1) < HALF

    def join(step, carry):
        for i in range(3):
            k = step * 3 + i
            for p in range(2):
                at = pl.multiple_of((p * windows + 2 * k) * span, span) + margin
                here = acc[pl.ds(at + span, low_rows), :]
                before = acc[pl.ds(at, low_rows), :]
                after = acc[pl.ds(at + 2 * span, low_rows), :]
                joined[pl.ds(p * low_rows * PITCH + k, low_rows, stride=PITCH), :] = here + jnp.where(
                    left, before, after
                )
        return carry

    lax.fori_loop(0, tiles // 3, join, 0)

    left32 = lax.broadcasted_iota(jnp.int32, (32, LANES), 1) < HALF
    zero = jnp.zeros((32, LANES), jnp.float32)
    counts_at = grid_rows * PITCH

    def counts(step, carry):
        here, before, after = carry
        for i in range(16):
            at = pl.multiple_of((step * 16 + i) * 64, 64)
            here = here + edge[pl.ds(at + 32, 32), :]
            before = before + edge[pl.ds(at, 32), :]
            after = after + edge[pl.ds(at + 1, 32), :]
            slot = counts_at + ((i & 1) * low_rows + step * 8 + (i >> 1)) * PITCH
            joined[pl.ds(slot, 32), :] = here + jnp.where(left32, before, after)
        return here, before, after

    lax.fori_loop(0, grid_rows // 16, counts, (zero, zero, zero))

    spot = lax.axis_index("frame")
    side = lax.axis_index("group")
    my_x, my_y, my_core = (side >> 1) * 2 + (spot & 1), spot >> 3, side & 1
    half_rows = keep.shape[0] // 2
    along_x = [device_of((my_x + d) & 3, 0, 0, 0) for d in range(4)]
    along_y = [device_of(0, (my_y + d) & 3, 0, 0) for d in range(4)]
    along_z = [device_of(0, 0, d, 0) for d in range(4)]
    last_field = len(entries)
    for ix in range(4):
        for iy in range(4):
            for iz in range(4):
                chip = along_x[ix] + along_y[iy] + along_z[iz]
                first_slot = (ix * 16 + iy * 4 + iz) * tiles
                second_slot = half_rows + (iy * 16 + ix * 4 + iz) * tiles
                for ref, core in ((keep, my_core), (send, 1 - my_core)):
                    at = table[last_field, 0, chip + core]
                    ref[first_slot : first_slot + tiles, :] = joined[pl.ds(at, tiles), :]
                    ref[second_slot : second_slot + tiles, :] = joined[pl.ds(counts_at + at, tiles), :]


def splat(frame, motion, weights, order):
    low_rows, low_cols = frame.shape
    grid_rows = 2 * low_rows
    tiles = 2 * low_cols // LANES
    windows = 2 * tiles + 2
    order = order.reshape(1, grid_rows)
    return pl.pallas_call(
        splat_kernel,
        out_shape=[jax.ShapeDtypeStruct((grid_rows * tiles, LANES), jnp.float32)] * 2,
        in_specs=[pl.BlockSpec(memory_space=pltpu.HBM)] * 4,
        out_specs=[pl.BlockSpec(memory_space=pltpu.VMEM)] * 2,
        scratch_shapes=[
            pltpu.VMEM(motion.shape, jnp.int32),
            pltpu.VMEM(weights.shape, jnp.int32),
            pltpu.VMEM(order.shape, jnp.int32),
            pltpu.VMEM(frame.shape, frame.dtype),
            pltpu.VMEM((8, 4, LANES), jnp.int32),
            pltpu.SMEM((8, 4, LANES), jnp.int32),
            pltpu.VMEM((tiles, low_rows + 16, LANES), jnp.float32),
            pltpu.VMEM((2 * windows * grid_rows, LANES), jnp.float32),
            pltpu.VMEM(((grid_rows + 2) * 64, LANES), jnp.float32),
            pltpu.VMEM((2 * grid_rows * PITCH, LANES), jnp.float32),
            pltpu.SemaphoreType.DMA((5,)),
        ],
        compiler_params=pltpu.CompilerParams(vmem_limit_bytes=32 * 1024 * 1024),
        name="splat",
    )(*(pltpu.with_memory_space_constraint(array, pltpu.HBM) for array in (motion, weights, order, frame)))


def split_kernel(parts, *refs):
    ins, outs = refs[: len(refs) - parts], refs[len(refs) - parts :]
    rows = outs[0].shape[0]
    for i, out in enumerate(outs):
        total = ins[0][i * rows : (i + 1) * rows, :]
        for ref in ins[1:]:
            total = total + ref[i * rows : (i + 1) * rows, :]
        out[...] = total


def fold(name, terms, parts):
    rows = terms[0].shape[0] // parts
    return pl.pallas_call(
        functools.partial(split_kernel, parts),
        out_shape=[jax.ShapeDtypeStruct((rows, LANES), jnp.float32)] * parts,
        in_specs=[pl.BlockSpec(memory_space=pltpu.VMEM)] * len(terms),
        out_specs=[pl.BlockSpec(memory_space=pltpu.VMEM)] * parts,
        compiler_params=pltpu.CompilerParams(vmem_limit_bytes=12 * 1024 * 1024),
        name=name,
    )(*terms)


def moved(value, dx, dy, dz, flip=0):
    pairs = []
    for x in range(4):
        for y in range(4):
            for z in range(4):
                for core in range(2):
                    pairs.append(
                        (device_of(x, y, z, core), device_of((x + dx) % 4, (y + dy) % 4, (z + dz) % 4, core ^ flip))
                    )
    return lax.ppermute(value, AXES, pairs)


def body(frames, motion, weights, strip_map, prior_image, prior_weight):
    tiles = 2 * frames.shape[2] // LANES
    keep, send = splat(frames[0], motion[0], weights[0], strip_map)
    other = moved(send, 0, 0, 0, flip=1)
    parts = fold("fold_core", [keep, other], 8)
    weighted, counted = list(parts[:4]), list(parts[4:])
    for d in range(1, 4):
        weighted[d] = moved(weighted[d], d, 0, 0)
        counted[d] = moved(counted[d], 0, d, 0)
    weighted = list(fold("fold_first", weighted, 4))
    counted = list(fold("fold_second", counted, 4))
    for d in range(1, 4):
        weighted[d] = moved(weighted[d], 0, d, 0)
        counted[d] = moved(counted[d], d, 0, 0)
    weighted = sum(weighted[1:], weighted[0]).reshape(4, tiles, LANES)
    counted = sum(counted[1:], counted[0]).reshape(4, tiles, LANES)
    both = jnp.concatenate([weighted, counted], axis=1)
    columns = [[device_of(x, y, z, c) for z in range(4)] for x in range(4) for y in range(4) for c in range(2)]
    total = lax.all_to_all(both, AXES, 0, 0, axis_index_groups=columns, tiled=True).sum(axis=0)
    sums = total[:tiles].reshape(prior_image.shape)
    counts = total[tiles:].reshape(prior_image.shape)
    return (sums + prior_weight * prior_image) / (counts + prior_weight)


def solution(mesh):
    in_specs = (
        P(AXES, None, None),
        P(AXES, None, None, None),
        P(AXES, None, None),
        P(),
        P(AXES, None, None),
        P(AXES, None, None),
    )
    return jax.shard_map(body, mesh=mesh, in_specs=in_specs, out_specs=P(AXES, None, None), check_vma=False)
```

```python
import functools

import jax
import jax.numpy as jnp
from jax import lax
from jax.experimental import pallas as pl
from jax.experimental.pallas import tpu as pltpu
from jax.sharding import PartitionSpec as P


MAX_SHIFT = 64
AXES = ("frame", "group")
LANES = 128
BLOCK = 32
HALF = 64
PITCH = 36


def device_of(x, y, z, core):
    return ((y * 4 + z) * 2 + (x & 1)) * 4 + (x >> 1) * 2 + core


def splat_kernel(
    motion_in, weights_in, order_in, frame_in, keep, send,
    motion, weights, order, frame, fields, table, low, acc, edge, joined, sems,
):
    low_rows, low_cols = frame.shape
    bands, blocks = weights.shape
    tiles = 2 * low_cols // LANES
    windows = 2 * tiles + 2
    grid_rows = 2 * low_rows
    span = grid_rows
    margin = MAX_SHIFT // 2
    copies = [
        pltpu.make_async_copy(source, target, sems.at[i])
        for i, (source, target) in enumerate(
            ((motion_in, motion), (weights_in, weights), (order_in, order), (frame_in, frame))
        )
    ]
    for copy in copies:
        copy.start()

    def clear(i, carry):
        for k in range(4):
            at = pl.multiple_of((i * 4 + k) * span, span) + margin
            acc[pl.ds(at, low_rows), :] = jnp.zeros((low_rows, LANES), jnp.float32)
        return carry

    lax.fori_loop(0, windows // 2, clear, 0)

    for copy in copies[:3]:
        copy.wait()
    band = lax.broadcasted_iota(jnp.int32, (bands, blocks), 0)
    block = lax.broadcasted_iota(jnp.int32, (bands, blocks), 1)
    dy, dx = motion[0], motion[1]
    window = (dx + BLOCK * block + HALF) >> 6
    par = dy & 1
    top = margin + 16 * band
    cell = (window & 1) * 32 + (window >> 1)
    entries = (
        (par * windows + window) * span + top + (dy >> 1),
        ((1 - par) * windows + window) * span + top + ((dy + 1) >> 1),
        dx & (LANES - 1),
        jnp.clip(BLOCK * band + dy, 0, grid_rows) * 64 + cell,
        jnp.clip(BLOCK * band + dy + BLOCK, 0, grid_rows) * 64 + cell,
        weights[...],
    )
    for f, entry in enumerate(entries):
        fields[f, :, :blocks] = entry
    row = order[...]
    fields[len(entries), :1, :] = ((row & 1) * low_rows + (row >> 1)) * PITCH

    def clear_edge(i, carry):
        at = pl.multiple_of(i * 512, 512)
        edge[pl.ds(at, 512), :] = jnp.zeros((512, LANES), jnp.float32)
        return carry

    lax.fori_loop(0, grid_rows * 64 // 512, clear_edge, 0)

    to_scalar = pltpu.make_async_copy(fields, table, sems.at[4])
    to_scalar.start()
    copies[3].wait()

    parts = low_cols // LANES
    cols = [frame[:, LANES * m : LANES * (m + 1)] for m in range(parts)]
    first = jnp.broadcast_to(frame[:, :1], (low_rows, LANES))
    last = jnp.broadcast_to(frame[:, low_cols - 1 :], (low_rows, LANES))
    source = jnp.concatenate(
        [jnp.concatenate([first] + cols[:-1], 0), jnp.concatenate(cols, 0), jnp.concatenate(cols[1:] + [last], 0)], 1
    )
    tap = lax.broadcasted_iota(jnp.int32, (3 * LANES, 2 * LANES), 0) - LANES
    target = lax.broadcasted_iota(jnp.int32, (3 * LANES, 2 * LANES), 1)
    near = target >> 1
    far = near + 2 * (target & 1) - 1
    stretch = jnp.where(tap == near, 0.75, jnp.where(tap == far, 0.25, 0.0)).astype(jnp.bfloat16)
    wide = jnp.dot(source, stretch, preferred_element_type=jnp.float32)
    for m in range(parts):
        for h in range(2):
            piece = wide[low_rows * m : low_rows * (m + 1), LANES * h : LANES * (h + 1)]
            low[2 * m + h, 8 : 8 + low_rows, :] = piece
            low[2 * m + h, 7:8, :] = piece[:1]
            low[2 * m + h, 8 + low_rows : 9 + low_rows, :] = piece[low_rows - 1 :]
    to_scalar.wait()

    owner = lax.broadcasted_iota(jnp.int32, (8, LANES), 1) // BLOCK

    def column(n, carry):
        for b in range(bands):
            base = 8 + 16 * b
            mid = 0.75 * low[n, base : base + 16, :]
            even = mid + 0.25 * low[n, base - 1 : base + 15, :]
            odd = mid + 0.25 * low[n, base + 1 : base + 17, :]
            for q in range(LANES // BLOCK):
                j = n * (LANES // BLOCK) + q
                at_even, at_odd, shift, at_first, at_end, w = (table[f, b, j] for f in range(6))
                gain = pltpu.roll(jnp.where(owner == q, w.astype(jnp.float32), 0.0), shift, 1)
                gains = jnp.concatenate([gain, gain], 0)
                acc[pl.ds(at_even, 16), :] += pltpu.roll(even, shift, 1) * gains
                acc[pl.ds(at_odd, 16), :] += pltpu.roll(odd, shift, 1) * gains
                edge[pl.ds(at_first, 1), :] += gain[:1]
                edge[pl.ds(at_end, 1), :] -= gain[:1]
        return carry

    lax.fori_loop(0, tiles, column, 0)

    left = lax.broadcasted_iota(jnp.int32, (low_rows, LANES), 1) < HALF

    def join(step, carry):
        for i in range(3):
            k = step * 3 + i
            for p in range(2):
                at = pl.multiple_of((p * windows + 2 * k) * span, span) + margin
                here = acc[pl.ds(at + span, low_rows), :]
                before = acc[pl.ds(at, low_rows), :]
                after = acc[pl.ds(at + 2 * span, low_rows), :]
                joined[pl.ds(p * low_rows * PITCH + k, low_rows, stride=PITCH), :] = here + jnp.where(
                    left, before, after
                )
        return carry

    lax.fori_loop(0, tiles // 3, join, 0)

    left32 = lax.broadcasted_iota(jnp.int32, (32, LANES), 1) < HALF
    zero = jnp.zeros((32, LANES), jnp.float32)
    counts_at = grid_rows * PITCH

    def counts(step, carry):
        here, before, after = carry
        for i in range(16):
            at = pl.multiple_of((step * 16 + i) * 64, 64)
            here = here + edge[pl.ds(at + 32, 32), :]
            before = before + edge[pl.ds(at, 32), :]
            after = after + edge[pl.ds(at + 1, 32), :]
            slot = counts_at + ((i & 1) * low_rows + step * 8 + (i >> 1)) * PITCH
            joined[pl.ds(slot, 32), :] = here + jnp.where(left32, before, after)
        return here, before, after

    lax.fori_loop(0, grid_rows // 16, counts, (zero, zero, zero))

    spot = lax.axis_index("frame")
    side = lax.axis_index("group")
    my_x, my_y, my_z, my_core = (side >> 1) * 2 + (spot & 1), spot >> 3, (spot >> 1) & 3, side & 1
    along_x = [device_of((my_x + d) & 3, 0, 0, 0) for d in range(4)]
    along_y = [device_of(0, (my_y + d) & 3, 0, 0) for d in range(4)]
    along_z = [device_of(0, 0, (my_z + d) & 3, 0) for d in range(4)]
    even_core = my_core == 0
    major = [jnp.where(even_core, x, y) for x, y in zip(along_x, along_y)]
    minor = [jnp.where(even_core, y, x) for x, y in zip(along_x, along_y)]
    kept_at = jnp.where(even_core, 0, counts_at)
    sent_at = counts_at - kept_at
    last_field = len(entries)
    for i1 in range(4):
        for i2 in range(4):
            for i3 in range(4):
                for flip in range(2):
                    slot = (((i1 * 4 + i2) * 4 + i3) * 2 + flip) * tiles
                    kept = major[i1] + minor[i2] + along_z[i3] + (my_core ^ flip)
                    sent = minor[i1] + major[i2] + along_z[i3] + (my_core ^ (1 - flip))
                    at = kept_at + table[last_field, 0, kept]
                    keep[slot : slot + tiles, :] = joined[pl.ds(at, tiles), :]
                    at = sent_at + table[last_field, 0, sent]
                    send[slot : slot + tiles, :] = joined[pl.ds(at, tiles), :]


def splat(frame, motion, weights, order):
    low_rows, low_cols = frame.shape
    grid_rows = 2 * low_rows
    tiles = 2 * low_cols // LANES
    windows = 2 * tiles + 2
    order = order.reshape(1, grid_rows)
    return pl.pallas_call(
        splat_kernel,
        out_shape=[jax.ShapeDtypeStruct((grid_rows * tiles, LANES), jnp.float32)] * 2,
        in_specs=[pl.BlockSpec(memory_space=pltpu.HBM)] * 4,
        out_specs=[pl.BlockSpec(memory_space=pltpu.VMEM)] * 2,
        scratch_shapes=[
            pltpu.VMEM(motion.shape, jnp.int32),
            pltpu.VMEM(weights.shape, jnp.int32),
            pltpu.VMEM(order.shape, jnp.int32),
            pltpu.VMEM(frame.shape, frame.dtype),
            pltpu.VMEM((8, 4, LANES), jnp.int32),
            pltpu.SMEM((8, 4, LANES), jnp.int32),
            pltpu.VMEM((tiles, low_rows + 16, LANES), jnp.float32),
            pltpu.VMEM((2 * windows * grid_rows, LANES), jnp.float32),
            pltpu.VMEM(((grid_rows + 2) * 64, LANES), jnp.float32),
            pltpu.VMEM((2 * grid_rows * PITCH, LANES), jnp.float32),
            pltpu.SemaphoreType.DMA((5,)),
        ],
        compiler_params=pltpu.CompilerParams(vmem_limit_bytes=32 * 1024 * 1024),
        name="splat",
    )(*(pltpu.with_memory_space_constraint(array, pltpu.HBM) for array in (motion, weights, order, frame)))


def split_kernel(parts, *refs):
    ins, outs = refs[: len(refs) - parts], refs[len(refs) - parts :]
    rows = outs[0].shape[0]
    for i, out in enumerate(outs):
        total = ins[0][i * rows : (i + 1) * rows, :]
        for ref in ins[1:]:
            total = total + ref[i * rows : (i + 1) * rows, :]
        out[...] = total


def fold(name, terms, parts):
    rows = terms[0].shape[0] // parts
    return pl.pallas_call(
        functools.partial(split_kernel, parts),
        out_shape=[jax.ShapeDtypeStruct((rows, LANES), jnp.float32)] * parts,
        in_specs=[pl.BlockSpec(memory_space=pltpu.VMEM)] * len(terms),
        out_specs=[pl.BlockSpec(memory_space=pltpu.VMEM)] * parts,
        compiler_params=pltpu.CompilerParams(vmem_limit_bytes=12 * 1024 * 1024),
        name=name,
    )(*terms)


def moved(value, stage, distance):
    pairs = []
    for x in range(4):
        for y in range(4):
            for z in range(4):
                for core in range(2):
                    at = [x, y, z]
                    if stage < 3:
                        axis = stage if stage == 2 or core == 0 else 1 - stage
                        at[axis] = (at[axis] + distance) % 4
                    pairs.append((device_of(x, y, z, core), device_of(*at, core if stage < 3 else 1 - core)))
    return lax.ppermute(value, AXES, pairs)


def body(frames, motion, weights, strip_map, prior_image, prior_weight):
    tiles = 2 * frames.shape[2] // LANES
    keep, send = splat(frames[0], motion[0], weights[0], strip_map)
    terms = [keep, moved(send, 3, 1)]
    for stage in range(3):
        parts = fold(f"fold_{stage}", terms, 4)
        terms = [parts[0]] + [moved(parts[d], stage, d) for d in range(1, 4)]
    total = sum(terms[1:], terms[0])
    mine, other = total[:tiles], total[tiles:]
    other = moved(other, 3, 1)
    even_core = (lax.axis_index("group") & 1) == 0
    sums = jnp.where(even_core, mine, other).reshape(prior_image.shape)
    counts = jnp.where(even_core, other, mine).reshape(prior_image.shape)
    return (sums + prior_weight * prior_image) / (counts + prior_weight)


def solution(mesh):
    in_specs = (
        P(AXES, None, None),
        P(AXES, None, None, None),
        P(AXES, None, None),
        P(),
        P(AXES, None, None),
        P(AXES, None, None),
    )
    return jax.shard_map(body, mesh=mesh, in_specs=in_specs, out_specs=P(AXES, None, None), check_vma=False)
```
